32 devices in a mesh: param: 16 (over z, x, core), qoi: 2 (over y).
Axes of the slice: x: 2, y: 2, z: 4, core: 2. Of those that a mesh axis runs over, the one named last changes fastest.
Arguments:
- samples: bfloat16 [16, 5120, 420], P('qoi', 'param'), may hold values from -6 to 6
- operator_rows: bfloat16 [8, 5120, 2, 512], P(None, 'param', None, 'qoi'), may hold values from -0.0625 to 0.0625
- block_start: int32 [1], replicated, may hold values from 0 to 203
- gauge_group: int32 [512], P('qoi'), may hold values from 0 to 15
Outputs:
- qoi_spectrum: float32 [16, 2, 8, 512], P('param', None, None, 'qoi')
- segment_response: float32 [16, 2, 8, 16], P('param')
The draws below stay inside these ranges and needn't reach their ends.
Inputs may be any that keep to these rules, and one draw needn't show every extreme that they name: `block_start`: the block's frequencies lie among the 211 frequencies of a real transform.
All inputs are finite; a program needn't handle non-finite values.
Results may differ from the reference program's by a relative error of at most 0.005.
Values may be sent and summed in bfloat16 or wider, within the bound.
No kernel may reach another device: no remote copies, remote signals or barrier semaphores. Data moves between devices by JAX's collectives and lax.ppermute only.
A program may use at most 64 MiB of HBM per device.

```python
import math
import jax
import jax.numpy as jnp
from jax import lax

NF = 8
NT = 420
GROUPS = 16
SAMPLES = 16
NP = 5120
GAUGES = 512


def place_ends(result, rng, least, largest):
    longest = result.shape.index(max(result.shape))
    spots = []
    for shift in (0, 1):
        where = [jax.random.randint(jax.random.fold_in(rng, axis), (), 0, length) for axis, length in enumerate(result.shape)]
        where[longest] = (where[longest] + shift) % result.shape[longest]
        spots.append(tuple(where))
    return result.at[spots[0]].set(least).at[spots[1]].set(largest)


def raised(result, own_key, source, target, shards_of, factor):
    owner, partner = [(jnp.arange(result.shape[dim]) // (result.shape[dim] // shards_of)).reshape([-1 if axis == dim else 1 for axis in range(result.ndim)]) for dim in (source, target)]
    chosen = jax.random.permutation(own_key, shards_of)[partner]
    strong = (owner == chosen) | (owner == (partner + shards_of // 2) % shards_of)
    return jnp.where(strong, factor * result, result)


def block_scale(own_key, extent, split, least, largest):
    def one(dim, shards_of):
        steps = jax.random.uniform(jax.random.fold_in(jax.random.fold_in(own_key, 6), dim), (shards_of,), jnp.float32, least / len(split), largest / len(split))
        return jnp.repeat(jnp.exp(steps), extent[dim] // shards_of).reshape((-1,) + (1,) * (len(extent) - dim - 1))

    loudness = one(*split[0])
    for cut in split[1:]:
        loudness = loudness * one(*cut)
    return loudness


def noise(rng, shape, width, most, shards=(), held_as=jnp.bfloat16):
    loudness = block_scale(rng, shape, shards, -0.22, 0.18) if shards else 1.0
    drawn = jax.random.normal(rng, shape, jnp.float32) * width * loudness
    return jnp.minimum(jnp.maximum(drawn, -most), most).astype(held_as)


def gaussian_with(key, dims, scale, reach, split, heavy, kind=jnp.bfloat16):
    array = scale * jax.random.normal(key, dims, jnp.float32)
    if split:
        array = array * block_scale(key, dims, split, -0.22, 0.18)
    return jnp.clip(raised(array, jax.random.fold_in(key, 3), *heavy), -reach, reach).astype(kind)


def setup_inputs(seed: int = 0) -> dict:
    key_of = jax.random.split(jax.random.key(seed), 5)
    return {
        "samples": gaussian_with(key_of[0], (SAMPLES, NP, NT), 1.0, 6.0, ((0, 2), (1, 16)), (1, 0, 16, 2.0)),
        "operator_rows": noise(key_of[1], (NF, NP, 2, GAUGES), (2 * NP) ** -0.5, 0.0625, ((1, 16), (3, 2))),
        "block_start": jax.random.randint(key_of[2], (1,), 0, NT // 2 + 2 - NF).astype(jnp.int32),
        "gauge_group": place_ends(jax.random.randint(key_of[3], (GAUGES,), 0, GROUPS), jax.random.fold_in(key_of[3], 1), 0, GROUPS - 1).astype(jnp.int32),
    }


def sample_spectrum(series, first):
    spectrum_all = jnp.fft.rfft(series.astype(jnp.float32), axis=-1)
    window = lax.dynamic_slice_in_dim(spectrum_all, first, NF, 1)
    factor = 1.0 / math.sqrt(NT)
    real_part = (jnp.real(window) * factor).astype(jnp.bfloat16)
    imag_part = (jnp.imag(window) * factor).astype(jnp.bfloat16)
    return jnp.stack([real_part, imag_part], axis=0)

def frequency_response(paired):
    spectrum_f, weights_f = paired
    real_w = weights_f[:, 0, :]
    imag_w = weights_f[:, 1, :]
    real_real = jnp.dot(spectrum_f[0], real_w, preferred_element_type=jnp.float32)
    imag_imag = jnp.dot(spectrum_f[1], imag_w, preferred_element_type=jnp.float32)
    real_imag = jnp.dot(spectrum_f[0], imag_w, preferred_element_type=jnp.float32)
    imag_real = jnp.dot(spectrum_f[1], real_w, preferred_element_type=jnp.float32)
    return jnp.stack([real_real - imag_imag, real_imag + imag_real], axis=0)

def reference(samples, operator_rows, block_start, gauge_group):
    first = block_start[0].astype(jnp.int32)
    spectra = lax.map(lambda series: sample_spectrum(series, first), samples)
    spectra = jnp.transpose(spectra, (3, 1, 0, 2))
    responses = lax.map(frequency_response, (spectra, operator_rows))
    qoi_spectrum = jnp.transpose(responses, (2, 1, 0, 3))
    onehot = (gauge_group[:, None] == jnp.arange(GROUPS, dtype=jnp.int32)[None, :]).astype(jnp.float32)
    segment = jnp.dot(qoi_spectrum.reshape(-1, GAUGES), onehot, precision=lax.Precision.HIGHEST, preferred_element_type=jnp.float32)
    segment_response = segment.reshape(SAMPLES, 2, NF, GROUPS) * math.sqrt(GROUPS / GAUGES)
    return (qoi_spectrum, segment_response)
```

```python
import math

import jax
import jax.numpy as jnp
from jax import lax
from jax.experimental import pallas as pl
from jax.experimental.pallas import tpu as pltpu
from jax.sharding import PartitionSpec as P

GROUPS = 16
ROWS = 8


def build_table(block_start, steps_count, freq_count, series_count):
    column = jnp.arange(steps_count * series_count, dtype=jnp.int32) // series_count
    freq_index = block_start[0] + jnp.arange(freq_count, dtype=jnp.int32)
    phase_index = freq_index[:, None] * column[None, :] % steps_count
    phases = phase_index.astype(jnp.float32) * (2.0 * math.pi / steps_count)
    table = jnp.concatenate([jnp.cos(phases), -jnp.sin(phases)], axis=0) / math.sqrt(steps_count)
    table_high = lax.optimization_barrier(table.astype(jnp.bfloat16)).astype(jnp.float32)
    table_low = (table - table_high).astype(jnp.bfloat16).astype(jnp.float32)
    return jnp.concatenate([table_high, table_low], axis=0)


def transform_kernel(table_ref, series_ref, spectrum_ref, spread_ref):
    table_rows, columns = table_ref.shape
    series_count = spread_ref.shape[0] // table_rows
    shape = (series_count, columns)
    own = lax.broadcasted_iota(jnp.int32, shape, 1) % series_count == lax.broadcasted_iota(
        jnp.int32, shape, 0
    )
    for row in range(0, table_rows, 2):
        pair = [
            jnp.where(own, jnp.broadcast_to(table_ref[one : one + 1, :], shape), 0.0)
            for one in (row, row + 1)
        ]
        spread_ref[row * series_count : (row + 2) * series_count, :] = jnp.concatenate(
            pair, axis=0
        ).astype(jnp.bfloat16)
    halves = jnp.dot(spread_ref[...], series_ref[...], preferred_element_type=jnp.float32)
    half = halves.shape[0] // 2
    spectrum_ref[...] = (halves[:half] + halves[half:]).astype(jnp.bfloat16)


def transform(samples, block_start, freq_count):
    series_count, param_local, steps_count = samples.shape
    table = build_table(block_start, steps_count, freq_count, series_count)
    series = samples.transpose(2, 0, 1).reshape(steps_count * series_count, param_local)
    rows = 2 * freq_count * series_count
    return pl.pallas_call(
        transform_kernel,
        out_shape=jax.ShapeDtypeStruct((rows, param_local), jnp.bfloat16),
        scratch_shapes=[pltpu.VMEM((2 * rows, steps_count * series_count), jnp.bfloat16)],
        name="transform",
    )(table, series)


def product_kernel(place_ref, weights_ref, *refs):
    *spectra_refs, terms_ref, ordered_ref, stage_ref = refs
    freq_count, param_local, _, gauge_local = weights_ref.shape
    parts = len(spectra_refs)
    series_count = spectra_refs[0].shape[0] // (2 * freq_count)
    for step, ref in enumerate(spectra_refs):
        ordered_ref[lax.rem(place_ref[0] + step, parts)] = ref[...]
    shape = (param_local, 2 * param_local)
    double = (
        lax.broadcasted_iota(jnp.int32, shape, 1) // 2 == lax.broadcasted_iota(jnp.int32, shape, 0)
    )
    double = jnp.where(double, 1.0, 0.0).astype(jnp.bfloat16)
    spread = [
        jnp.dot(ordered_ref[part], double, preferred_element_type=jnp.float32)
        for part in range(parts)
    ]
    even = lax.broadcasted_iota(jnp.int32, (parts * series_count, 2 * param_local), 1) % 2 == 0
    for freq in range(freq_count):
        real, imag = [
            jnp.concatenate(
                [
                    one[(kind * freq_count + freq) * series_count :][:series_count]
                    for one in spread
                ],
                axis=0,
            )
            for kind in (0, 1)
        ]
        rows = jnp.concatenate(
            [jnp.where(even, real, -imag), jnp.where(even, imag, real)], axis=0
        ).astype(jnp.bfloat16)
        weights = weights_ref[freq].reshape(2 * param_local, gauge_local)
        product = jnp.dot(rows, weights, preferred_element_type=jnp.float32)
        half = parts * series_count
        stage_ref[:, 0, freq, :] = product[:half]
        stage_ref[:, 1, freq, :] = product[half:]
    terms_ref[...] = stage_ref[...].astype(jnp.bfloat16)


def exchange(own, axis):
    count = lax.axis_size(axis)
    moved = [own]
    for step in range(1, count):
        pairs = [(source, (source - step) % count) for source in range(count)]
        moved.append(lax.ppermute(own, axis, pairs))
    return moved


def products(spectrum, operator_rows):
    freq_count, param_local, _, gauge_local = operator_rows.shape
    spectra = exchange(spectrum, "qoi")
    place = lax.axis_index("qoi").astype(jnp.int32).reshape(1)
    samples_total = len(spectra) * spectrum.shape[0] // (2 * freq_count)
    shape = (samples_total, 2, freq_count, gauge_local)
    return pl.pallas_call(
        product_kernel,
        in_specs=[pl.BlockSpec(memory_space=pltpu.SMEM)]
        + [pl.BlockSpec(memory_space=pltpu.VMEM)] * (1 + len(spectra)),
        out_shape=jax.ShapeDtypeStruct(shape, jnp.bfloat16),
        scratch_shapes=[
            pltpu.VMEM((len(spectra),) + spectrum.shape, jnp.bfloat16),
            pltpu.VMEM(shape, jnp.float32),
        ],
        name="products",
    )(place, operator_rows, *spectra)


def scatter_sum(terms, stride, count):
    total = lax.axis_size("param")
    member = lax.axis_index("param") // stride % count
    moved = []
    for step in range(1, count):
        pairs = []
        for source in range(total):
            place = source // stride % count
            pairs.append((source, source + ((place + step) % count - place) * stride))
        chunk = lax.dynamic_index_in_dim(terms, (member + step) % count, 0, keepdims=False)
        moved.append(lax.ppermute(chunk.astype(jnp.bfloat16), "param", pairs))
    result = lax.dynamic_index_in_dim(terms, member, 0, keepdims=False).astype(jnp.float32)
    for one in moved:
        result = result + one.astype(jnp.float32)
    return result


def local(samples, operator_rows, block_start, gauge_group):
    freq_count = operator_rows.shape[0]
    gauge_local = operator_rows.shape[3]
    terms = products(transform(samples, block_start, freq_count), operator_rows)
    param_count = lax.axis_size("param")
    own_rows = terms.shape[0] // param_count
    inner = 4 if param_count % 4 == 0 else 1
    outer = param_count // inner
    rest = (own_rows, 2, freq_count, gauge_local)
    half_sums = scatter_sum(terms.reshape((outer, inner) + rest), inner, outer)
    qoi_spectrum = scatter_sum(half_sums, 1, inner)
    onehot = (gauge_group[:, None] == jnp.arange(GROUPS, dtype=jnp.int32)[None, :]).astype(
        jnp.float32
    )
    local_sums = jnp.dot(
        qoi_spectrum.reshape(-1, gauge_local),
        onehot,
        precision=lax.Precision.HIGHEST,
        preferred_element_type=jnp.float32,
    )
    local_sums = local_sums.reshape(own_rows, 2, freq_count, GROUPS)
    summed = sum(exchange(local_sums, "qoi"))
    norm_factor = math.sqrt(GROUPS / (gauge_local * lax.axis_size("qoi")))
    return (qoi_spectrum, summed * norm_factor)


def solution(mesh):
    return jax.shard_map(
        local,
        mesh=mesh,
        in_specs=(P("qoi", "param", None), P(None, "param", None, "qoi"), P(), P("qoi")),
        out_specs=(P("param", None, None, "qoi"), P("param", None, None, None)),
        check_vma=False,
    )
```

```python
import math

import jax
import jax.numpy as jnp
from jax import lax
from jax.experimental import pallas as pl
from jax.experimental.pallas import tpu as pltpu
from jax.sharding import PartitionSpec as P

GROUPS = 16
SCOPED = 24 << 20
SINE = (-1 / 6, 1 / 120, -1 / 5040, 1 / 362880, -1 / 39916800, 1 / 6227020800)


def quarter_sine(turns):
    angle = turns * (2.0 * math.pi)
    square = angle * angle
    series = jnp.full_like(square, SINE[-1])
    for term in SINE[-2::-1]:
        series = series * square + term
    return angle + angle * square * series


def transform_kernel(start_ref, series_ref, spectrum_ref, table_ref, spread_ref, held_ref, sem):
    table_rows, columns = table_ref.shape
    freq_count = table_rows // 4
    series_count = spread_ref.shape[0] // table_rows
    steps_count = columns // series_count
    copy = pltpu.make_async_copy(series_ref, held_ref, sem)
    copy.start()
    table_shape = (freq_count, columns)
    step = (lax.broadcasted_iota(jnp.int32, table_shape, 1) // series_count).astype(jnp.float32)
    freq = (start_ref[0] + lax.broadcasted_iota(jnp.int32, table_shape, 0)).astype(jnp.float32)
    phase = step * freq
    phase = phase - jnp.floor(phase * (1.0 / steps_count) + 0.5) * steps_count
    near = jnp.where(phase > steps_count / 4, steps_count / 2 - phase, phase)
    near = jnp.where(phase < -steps_count / 4, -steps_count / 2 - phase, near)
    scale = 1.0 / math.sqrt(steps_count)
    cosine = quarter_sine((steps_count / 4 - jnp.abs(phase)) / steps_count) * scale
    sine = quarter_sine(near / steps_count) * -scale
    for kind, value in enumerate((cosine, sine)):
        high = value.astype(jnp.bfloat16).astype(jnp.float32)
        table_ref[kind * freq_count : (kind + 1) * freq_count, :] = high
        table_ref[(kind + 2) * freq_count : (kind + 3) * freq_count, :] = value - high
    shape = (series_count, columns)
    own = lax.broadcasted_iota(jnp.int32, shape, 1) % series_count == lax.broadcasted_iota(
        jnp.int32, shape, 0
    )
    for row in range(0, table_rows, 2):
        pair = [
            jnp.where(own, jnp.broadcast_to(table_ref[one : one + 1, :], shape), 0.0)
            for one in (row, row + 1)
        ]
        spread_ref[row * series_count : (row + 2) * series_count, :] = jnp.concatenate(
            pair, axis=0
        ).astype(jnp.bfloat16)
    copy.wait()
    halves = jnp.dot(spread_ref[...], held_ref[...], preferred_element_type=jnp.float32)
    half = halves.shape[0] // 2
    spectrum_ref[...] = (halves[:half] + halves[half:]).astype(jnp.bfloat16)


def transform(samples, block_start, freq_count):
    series_count, param_local, steps_count = samples.shape
    series = samples.transpose(2, 0, 1).reshape(steps_count * series_count, param_local)
    rows = 2 * freq_count * series_count
    return pl.pallas_call(
        transform_kernel,
        in_specs=[pl.BlockSpec(memory_space=pltpu.SMEM), pl.BlockSpec(memory_space=pl.ANY)],
        out_shape=pltpu.VMEM((rows, param_local), jnp.bfloat16),
        scratch_shapes=[
            pltpu.VMEM((4 * freq_count, steps_count * series_count), jnp.float32),
            pltpu.VMEM((2 * rows, steps_count * series_count), jnp.bfloat16),
            pltpu.VMEM(series.shape, series.dtype),
            pltpu.SemaphoreType.DMA,
        ],
        compiler_params=pltpu.CompilerParams(vmem_limit_bytes=SCOPED),
        name="transform",
    )(block_start, series)


def product_of(spectrum_ref, weights_ref, stage_ref):
    freq_count, param_local, _, gauge_local = weights_ref.shape
    series_count = spectrum_ref.shape[0] // (2 * freq_count)
    shape = (param_local, 2 * param_local)
    double = (
        lax.broadcasted_iota(jnp.int32, shape, 1) // 2 == lax.broadcasted_iota(jnp.int32, shape, 0)
    )
    double = jnp.where(double, 1.0, 0.0).astype(jnp.bfloat16)
    spread = jnp.dot(spectrum_ref[...], double, preferred_element_type=jnp.float32)
    even = lax.broadcasted_iota(jnp.int32, (series_count, 2 * param_local), 1) % 2 == 0
    for freq in range(freq_count):
        real, imag = [
            spread[(kind * freq_count + freq) * series_count :][:series_count] for kind in (0, 1)
        ]
        rows = jnp.concatenate(
            [jnp.where(even, real, -imag), jnp.where(even, imag, real)], axis=0
        ).astype(jnp.bfloat16)
        weights = weights_ref[freq].reshape(2 * param_local, gauge_local)
        product = jnp.dot(rows, weights, preferred_element_type=jnp.float32)
        stage_ref[:, 0, freq, :] = product[:series_count]
        stage_ref[:, 1, freq, :] = product[series_count:]
    return stage_ref[...].astype(jnp.bfloat16)


def own_kernel(weights_ref, spectrum_ref, terms_ref, stage_ref):
    terms_ref[...] = product_of(spectrum_ref, weights_ref, stage_ref)


def other_kernel(place_ref, weights_ref, own_ref, *refs):
    *spectra_refs, terms_ref, stage_ref = refs
    parts = len(spectra_refs) + 1
    terms_ref[place_ref[0]] = own_ref[...]
    for step, ref in enumerate(spectra_refs):
        terms_ref[lax.rem(place_ref[0] + step + 1, parts)] = product_of(ref, weights_ref, stage_ref)


def exchange(own, axis):
    count = lax.axis_size(axis)
    moved = [own]
    for step in range(1, count):
        pairs = [(source, (source - step) % count) for source in range(count)]
        moved.append(lax.ppermute(own, axis, pairs))
    return moved


def in_fast(value):
    return pltpu.with_memory_space_constraint(value, pltpu.VMEM)


def products(spectrum, operator_rows):
    freq_count, param_local, _, gauge_local = operator_rows.shape
    weights = in_fast(operator_rows)
    spectra = [in_fast(one) for one in exchange(spectrum, "qoi")]
    place = lax.axis_index("qoi").astype(jnp.int32).reshape(1)
    series_count = spectrum.shape[0] // (2 * freq_count)
    shape = (series_count, 2, freq_count, gauge_local)
    work = 8 * series_count * param_local * freq_count * gauge_local
    in_vmem = pl.BlockSpec(memory_space=pltpu.VMEM)
    own = pl.pallas_call(
        own_kernel,
        in_specs=[in_vmem] * 2,
        out_shape=pltpu.VMEM(shape, jnp.bfloat16),
        scratch_shapes=[pltpu.VMEM(shape, jnp.float32)],
        cost_estimate=pl.CostEstimate(flops=8 * work, bytes_accessed=weights.size, transcendentals=0),
        compiler_params=pltpu.CompilerParams(vmem_limit_bytes=SCOPED),
        name="own_products",
    )(weights, spectra[0])
    if len(spectra) == 1:
        return own
    terms = pl.pallas_call(
        other_kernel,
        in_specs=[pl.BlockSpec(memory_space=pltpu.SMEM)] + [in_vmem] * (1 + len(spectra)),
        out_shape=pltpu.VMEM((len(spectra),) + shape, jnp.bfloat16),
        scratch_shapes=[pltpu.VMEM(shape, jnp.float32)],
        compiler_params=pltpu.CompilerParams(vmem_limit_bytes=SCOPED),
        name="other_products",
    )(place, weights, in_fast(own), *spectra[1:])
    return terms.reshape((len(spectra) * series_count,) + shape[1:])


def scatter_sum(terms, stride, count):
    total = lax.axis_size("param")
    member = lax.axis_index("param") // stride % count
    moved = []
    for step in range(1, count):
        pairs = []
        for source in range(total):
            place = source // stride % count
            pairs.append((source, source + ((place + step) % count - place) * stride))
        chunk = lax.dynamic_index_in_dim(terms, (member + step) % count, 0, keepdims=False)
        moved.append(lax.ppermute(chunk.astype(jnp.bfloat16), "param", pairs))
    result = lax.dynamic_index_in_dim(terms, member, 0, keepdims=False).astype(jnp.float32)
    for one in moved:
        result = result + one.astype(jnp.float32)
    return result


def local(samples, operator_rows, block_start, gauge_group):
    freq_count = operator_rows.shape[0]
    gauge_local = operator_rows.shape[3]
    terms = products(transform(samples, block_start, freq_count), operator_rows)
    param_count = lax.axis_size("param")
    own_rows = terms.shape[0] // param_count
    inner = 4 if param_count % 4 == 0 else 1
    outer = param_count // inner
    rest = (own_rows, 2, freq_count, gauge_local)
    half_sums = scatter_sum(terms.reshape((outer, inner) + rest), inner, outer)
    qoi_spectrum = scatter_sum(half_sums, 1, inner)
    onehot = (gauge_group[:, None] == jnp.arange(GROUPS, dtype=jnp.int32)[None, :]).astype(
        jnp.float32
    )
    local_sums = jnp.dot(
        qoi_spectrum.reshape(-1, gauge_local),
        onehot,
        precision=lax.Precision.HIGHEST,
        preferred_element_type=jnp.float32,
    )
    local_sums = local_sums.reshape(own_rows, 2, freq_count, GROUPS)
    summed = sum(exchange(local_sums, "qoi"))
    norm_factor = math.sqrt(GROUPS / (gauge_local * lax.axis_size("qoi")))
    return (qoi_spectrum, summed * norm_factor)


def solution(mesh):
    return jax.shard_map(
        local,
        mesh=mesh,
        in_specs=(P("qoi", "param", None), P(None, "param", None, "qoi"), P(), P("qoi")),
        out_specs=(P("param", None, None, "qoi"), P("param", None, None, None)),
        check_vma=False,
    )
```

```python
import math

import jax
import jax.numpy as jnp
from jax import lax
from jax.experimental import pallas as pl
from jax.experimental.pallas import tpu as pltpu
from jax.sharding import PartitionSpec as P

GROUPS = 16
SCOPED = 24 << 20
SINE = (-1 / 6, 1 / 120, -1 / 5040, 1 / 362880, -1 / 39916800, 1 / 6227020800)


def quarter_sine(turns):
    angle = turns * (2.0 * math.pi)
    square = angle * angle
    series = jnp.full_like(square, SINE[-1])
    for term in SINE[-2::-1]:
        series = series * square + term
    return angle + angle * square * series


def transform_kernel(
    start_ref, series_ref, spectrum_ref, table_ref, spread_ref, held_ref, sem
):
    table_rows, columns = table_ref.shape
    freq_count = table_rows // 4
    series_count = spread_ref.shape[0] // table_rows
    steps_count = columns // series_count
    copy = pltpu.make_async_copy(series_ref, held_ref, sem)
    copy.start()
    table_shape = (freq_count, columns)
    step = (lax.broadcasted_iota(jnp.int32, table_shape, 1) // series_count).astype(jnp.float32)
    freq = (start_ref[0] + lax.broadcasted_iota(jnp.int32, table_shape, 0)).astype(jnp.float32)
    phase = step * freq
    phase = phase - jnp.floor(phase * (1.0 / steps_count) + 0.5) * steps_count
    near = jnp.where(phase > steps_count / 4, steps_count / 2 - phase, phase)
    near = jnp.where(phase < -steps_count / 4, -steps_count / 2 - phase, near)
    scale = 1.0 / math.sqrt(steps_count)
    cosine = quarter_sine((steps_count / 4 - jnp.abs(phase)) / steps_count) * scale
    sine = quarter_sine(near / steps_count) * -scale
    for kind, value in enumerate((cosine, sine)):
        high = value.astype(jnp.bfloat16).astype(jnp.float32)
        table_ref[kind * freq_count : (kind + 1) * freq_count, :] = high
        table_ref[(kind + 2) * freq_count : (kind + 3) * freq_count, :] = value - high
    shape = (series_count, columns)
    own = lax.broadcasted_iota(jnp.int32, shape, 1) % series_count == lax.broadcasted_iota(
        jnp.int32, shape, 0
    )
    for row in range(0, table_rows, 2):
        pair = [
            jnp.where(own, jnp.broadcast_to(table_ref[one : one + 1, :], shape), 0.0)
            for one in (row, row + 1)
        ]
        spread_ref[row * series_count : (row + 2) * series_count, :] = jnp.concatenate(
            pair, axis=0
        ).astype(jnp.bfloat16)
    copy.wait()
    halves = jnp.dot(spread_ref[...], held_ref[...], preferred_element_type=jnp.float32)
    half = halves.shape[0] // 2
    spectrum_ref[...] = (halves[:half] + halves[half:]).astype(jnp.bfloat16)


def transform(samples, block_start, freq_count):
    series_count, param_local, steps_count = samples.shape
    series = samples.transpose(2, 0, 1).reshape(steps_count * series_count, param_local)
    series = pltpu.with_memory_space_constraint(series, pltpu.HBM)
    rows = 2 * freq_count * series_count
    return pl.pallas_call(
        transform_kernel,
        in_specs=[pl.BlockSpec(memory_space=pltpu.SMEM), pl.BlockSpec(memory_space=pltpu.HBM)],
        out_shape=pltpu.VMEM((rows, param_local), jnp.bfloat16),
        scratch_shapes=[
            pltpu.VMEM((4 * freq_count, steps_count * series_count), jnp.float32),
            pltpu.VMEM((2 * rows, steps_count * series_count), jnp.bfloat16),
            pltpu.VMEM(series.shape, series.dtype),
            pltpu.SemaphoreType.DMA,
        ],
        compiler_params=pltpu.CompilerParams(vmem_limit_bytes=SCOPED),
        name="transform",
    )(block_start, series)


def product_of(spectrum_ref, weights_ref, stage_ref, copies=()):
    freq_count, param_local, _, gauge_local = weights_ref.shape
    series_count = spectrum_ref.shape[0] // (2 * freq_count)
    shape = (param_local, 2 * param_local)
    double = (
        lax.broadcasted_iota(jnp.int32, shape, 1) // 2 == lax.broadcasted_iota(jnp.int32, shape, 0)
    )
    double = jnp.where(double, 1.0, 0.0).astype(jnp.bfloat16)
    spread = jnp.dot(spectrum_ref[...], double, preferred_element_type=jnp.float32)
    even = lax.broadcasted_iota(jnp.int32, (series_count, 2 * param_local), 1) % 2 == 0
    for freq in range(freq_count):
        real, imag = [
            spread[(kind * freq_count + freq) * series_count :][:series_count] for kind in (0, 1)
        ]
        rows = jnp.concatenate(
            [jnp.where(even, real, -imag), jnp.where(even, imag, real)], axis=0
        ).astype(jnp.bfloat16)
        if copies:
            copies[freq].wait()
        weights = weights_ref[freq].reshape(2 * param_local, gauge_local)
        product = jnp.dot(rows, weights, preferred_element_type=jnp.float32)
        stage_ref[:, 0, freq, :] = product[:series_count]
        stage_ref[:, 1, freq, :] = product[series_count:]
    return stage_ref[...].astype(jnp.bfloat16)


def own_kernel(weights_ref, spectrum_ref, terms_ref, held_ref, stage_ref, sems):
    copies = [
        pltpu.make_async_copy(weights_ref.at[freq], held_ref.at[freq], sems.at[freq])
        for freq in range(weights_ref.shape[0])
    ]
    for copy in copies:
        copy.start()
    terms_ref[...] = product_of(spectrum_ref, held_ref, stage_ref, copies)


def other_kernel(place_ref, weights_ref, own_ref, *refs):
    *spectra_refs, terms_ref, stage_ref = refs
    parts = len(spectra_refs) + 1
    terms_ref[place_ref[0]] = own_ref[...]
    for step, ref in enumerate(spectra_refs):
        terms_ref[lax.rem(place_ref[0] + step + 1, parts)] = product_of(ref, weights_ref, stage_ref)


def exchange(own, axis):
    count = lax.axis_size(axis)
    moved = [own]
    for step in range(1, count):
        pairs = [(source, (source - step) % count) for source in range(count)]
        moved.append(lax.ppermute(own, axis, pairs))
    return moved


def in_fast(value):
    return pltpu.with_memory_space_constraint(value, pltpu.VMEM)


def products(spectrum, operator_rows):
    freq_count, param_local, _, gauge_local = operator_rows.shape
    spectra = [in_fast(one) for one in exchange(spectrum, "qoi")]
    place = lax.axis_index("qoi").astype(jnp.int32).reshape(1)
    series_count = spectrum.shape[0] // (2 * freq_count)
    shape = (series_count, 2, freq_count, gauge_local)
    work = 8 * series_count * param_local * freq_count * gauge_local
    in_vmem = pl.BlockSpec(memory_space=pltpu.VMEM)
    own, weights = pl.pallas_call(
        own_kernel,
        in_specs=[pl.BlockSpec(memory_space=pl.ANY), in_vmem],
        out_shape=(
            pltpu.VMEM(shape, jnp.bfloat16),
            pltpu.VMEM(operator_rows.shape, operator_rows.dtype),
        ),
        scratch_shapes=[pltpu.VMEM(shape, jnp.float32), pltpu.SemaphoreType.DMA((freq_count,))],
        cost_estimate=pl.CostEstimate(flops=8 * work, bytes_accessed=operator_rows.size, transcendentals=0),
        compiler_params=pltpu.CompilerParams(vmem_limit_bytes=SCOPED),
        name="own_products",
    )(operator_rows, spectra[0])
    if len(spectra) == 1:
        return own
    terms = pl.pallas_call(
        other_kernel,
        in_specs=[pl.BlockSpec(memory_space=pltpu.SMEM)] + [in_vmem] * (1 + len(spectra)),
        out_shape=pltpu.VMEM((len(spectra),) + shape, jnp.bfloat16),
        scratch_shapes=[pltpu.VMEM(shape, jnp.float32)],
        compiler_params=pltpu.CompilerParams(vmem_limit_bytes=SCOPED),
        name="other_products",
    )(place, in_fast(weights), in_fast(own), *spectra[1:])
    return terms.reshape((len(spectra) * series_count,) + shape[1:])


def scatter_sum(terms, stride, count):
    total = lax.axis_size("param")
    member = lax.axis_index("param") // stride % count
    moved = []
    mirrored = count & (count - 1) == 0
    for step in range(1, count):
        pairs = []
        for source in range(total):
            place = source // stride % count
            target = place ^ step if mirrored else (place + step) % count
            pairs.append((source, source + (target - place) * stride))
        target = member ^ step if mirrored else (member + step) % count
        chunk = lax.dynamic_index_in_dim(terms, target, 0, keepdims=False)
        moved.append(lax.ppermute(chunk.astype(jnp.bfloat16), "param", pairs))
    result = lax.dynamic_index_in_dim(terms, member, 0, keepdims=False).astype(jnp.float32)
    for one in moved:
        result = result + one.astype(jnp.float32)
    return result


def local(samples, operator_rows, block_start, gauge_group):
    freq_count = operator_rows.shape[0]
    gauge_local = operator_rows.shape[3]
    terms = products(transform(samples, block_start, freq_count), operator_rows)
    param_count = lax.axis_size("param")
    own_rows = terms.shape[0] // param_count
    inner = 4 if param_count % 4 == 0 else 1
    outer = param_count // inner
    rest = (own_rows, 2, freq_count, gauge_local)
    half_sums = scatter_sum(terms.reshape((outer, inner) + rest), inner, outer)
    qoi_spectrum = scatter_sum(half_sums, 1, inner)
    onehot = (gauge_group[:, None] == jnp.arange(GROUPS, dtype=jnp.int32)[None, :]).astype(
        jnp.float32
    )
    local_sums = jnp.dot(
        qoi_spectrum.reshape(-1, gauge_local),
        onehot,
        precision=lax.Precision.HIGHEST,
        preferred_element_type=jnp.float32,
    )
    local_sums = local_sums.reshape(own_rows, 2, freq_count, GROUPS)
    summed = sum(exchange(local_sums, "qoi"))
    norm_factor = math.sqrt(GROUPS / (gauge_local * lax.axis_size("qoi")))
    return (qoi_spectrum, summed * norm_factor)


def solution(mesh):
    return jax.shard_map(
        local,
        mesh=mesh,
        in_specs=(P("qoi", "param", None), P(None, "param", None, "qoi"), P(), P("qoi")),
        out_specs=(P("param", None, None, "qoi"), P("param", None, None, None)),
        check_vma=False,
    )
```
